32 devices in a mesh: patch: 8 (over z, y), sub: 4 (over x, core).
Axes of the slice: x: 2, y: 2, z: 4, core: 2. Of those that a mesh axis runs over, the one named last changes fastest.
Arguments:
- heat: float32 [262144], P(('patch', 'sub')), may hold values from -6 to 6
- basis: bfloat16 [9, 524288], P(None, ('patch', 'sub')), may hold values from -3 to 3
- area: float32 [524288], P(('patch', 'sub')), may hold values from 0.2 to 2
- corners: int32 [3, 524288], P(None, ('patch', 'sub')), may hold values from 0 to 9215, as said below
- send_sub: int32 [4096], P(('patch', 'sub')), may hold values from 0 to 8191
- send_pat: int32 [4, 4096], P(None, ('patch', 'sub')), may hold values from 0 to 8191
- live_faces: int32 [32], P(('patch', 'sub')), may hold values from 12288 to 16384, as said below
Outputs:
- divergence: float32 [262144], P(('patch', 'sub'))
The draws below stay inside these ranges and needn't reach their ends.
Inputs may be any that keep to these rules, and one draw needn't show every extreme that they name: Face slot f of a device lies in tile t = f // 128; each of its corners is either an owned position in [64 t - 128, 64 t + 128) or a remote position from 8192 + 256 (t mod (4)) up to 255 beyond that; every position of the device's table is read by some face of the device. `live_faces`: some device has all 16384 slots live.
All inputs are finite; a program needn't handle non-finite values.
Results may differ from the reference program's by a relative error of at most 0.0003.
Values sent between devices are 32-bit elements; how exact they have to be, the bound alone decides.
A program may use at most 64 MiB of HBM per device.

```python
import math
import jax
import jax.numpy as jnp
from jax import lax

V_DEV = 8192
F_DEV = 16384
S_SUB = 128
S_PAT = 128
RADIUS = 2
VERTS = 262144
FACES = 524288
GROUP_SENDS = 4096
PATCH_SENDS = 4096
N_PATCH = 8
N_SUB = 4


def draw_corners(key, part):
    devices = N_PATCH * N_SUB
    remote_len = N_SUB * S_SUB + 2 * RADIUS * S_PAT
    remote_win = min(256, remote_len)
    remote_blocks = remote_len // remote_win
    tiles = F_DEV // 128
    slot = jnp.arange(F_DEV).astype(jnp.int32)
    tile = slot // 128
    inner = slot % 128

    def one_device(device_key):
        keys = jax.random.split(device_key, 6)
        tile_keys = jax.random.split(keys[0], tiles)
        orders = jax.vmap(lambda single: jax.random.permutation(single, 64))(tile_keys).astype(jnp.int32)
        first = 64 * tile + orders[tile, inner % 64]
        lower = jnp.maximum(0, 64 * (tile - 2))
        upper = jnp.minimum(V_DEV, 64 * (tile + 2))
        near_one = jax.random.randint(keys[1], (F_DEV,), lower, upper).astype(jnp.int32)
        near_two = jax.random.randint(keys[2], (F_DEV,), lower, upper).astype(jnp.int32)
        remote_order = jax.random.permutation(keys[3], remote_win).astype(jnp.int32)
        counter = tile // remote_blocks * 32 + inner // 4
        remote_base = V_DEV + remote_win * (tile % remote_blocks)
        far_one = remote_base + remote_order[counter % remote_win]
        far_two = remote_base + jax.random.randint(keys[4], (F_DEV,), 0, remote_win).astype(jnp.int32)
        flagged = jax.random.randint(keys[5], (F_DEV,), 0, 8) == 0
        second = jnp.where(inner % 4 == 0, far_one, near_one)
        third = jnp.where(flagged, far_two, near_two)
        return jnp.stack([first, second, third]).astype(jnp.int32)
    device_keys = jax.random.split(jax.random.fold_in(key, 11), devices)
    positions = jax.vmap(one_device)(device_keys)
    return positions.transpose(1, 0, 2).reshape(3, devices * F_DEV).astype(jnp.int32)


def draw_live_faces(key, part):
    devices = N_PATCH * N_SUB
    first, second = jax.random.split(jax.random.fold_in(key, 23))
    counts = jax.random.randint(first, (devices,), 3 * F_DEV // 4, F_DEV + 1).astype(jnp.int32)
    fullest = jax.random.randint(second, (), 0, devices)
    return jnp.where(jnp.arange(devices) == fullest, F_DEV, counts).astype(jnp.int32)


def place_ends(array, own_key, smallest, top_value):
    longest = array.shape.index(max(array.shape))
    spots = []
    for shift in (0, 1):
        where = [jax.random.randint(jax.random.fold_in(own_key, axis), (), 0, length) for axis, length in enumerate(array.shape)]
        where[longest] = (where[longest] + shift) % array.shape[longest]
        spots.append(tuple(where))
    return array.at[spots[0]].set(smallest).at[spots[1]].set(top_value)


def shard_levels(own_key, extent, cuts, least, top_value):
    factor_of, own = 1.0, jax.random.fold_in(own_key, 6)
    for position, shards_of in cuts:
        steps = jnp.exp(jax.random.uniform(jax.random.fold_in(own, position), (shards_of,), jnp.float32, least / len(cuts), top_value / len(cuts)))
        factor_of = factor_of * jnp.repeat(steps, extent[position] // shards_of).reshape([-1 if axis == position else 1 for axis in range(len(extent))])
    return factor_of


def centred(rng, dims, scale, bound, shards=(), dtype=jnp.bfloat16):
    level = shard_levels(rng, dims, shards, -0.22, 0.18) if shards else 1.0
    values = jax.random.normal(rng, dims, jnp.float32) * scale * level
    return jnp.minimum(jnp.maximum(values, -bound), bound).astype(dtype)


def setup_inputs(seed: int = 0) -> dict:
    splits = jax.random.split(jax.random.key(seed), 8)
    return {
        "heat": centred(splits[0], (VERTS,), 1.0, 6.0, ((0, 32),), jnp.float32),
        "basis": centred(splits[1], (9, FACES), 0.5, 3.0, ((1, 32),)),
        "area": jnp.clip(jnp.exp(math.log(2.0) - 2.3025851 * jax.random.uniform(splits[2], (FACES,), jnp.float32) ** shard_levels(splits[2], (FACES,), ((0, 32),), -0.2, 0.2)), 0.2, 2.0),
        "corners": draw_corners(jax.random.fold_in(splits[7], 71), 0),
        "send_sub": place_ends(jax.random.randint(splits[4], (GROUP_SENDS,), 0, V_DEV), jax.random.fold_in(splits[4], 1), 0, V_DEV - 1).astype(jnp.int32),
        "send_pat": place_ends(jax.random.randint(splits[5], (2 * RADIUS, PATCH_SENDS), 0, V_DEV), jax.random.fold_in(splits[5], 1), 0, V_DEV - 1).astype(jnp.int32),
        "live_faces": draw_live_faces(jax.random.fold_in(splits[7], 71), 0),
    }


def offset_list():
    return [k + 1 for k in range(RADIUS)] + [-(k + 1) for k in range(RADIUS)]

def face_terms(lookup_table, corner_ids, basis_dev, area_dev, live_count):
    slots = corner_ids.shape[1]
    values = lookup_table[corner_ids]
    gradients = basis_dev.astype(jnp.float32).reshape(3, 3, slots)
    gradient = lax.optimization_barrier(jnp.sum(gradients * values[:, None, :], axis=0))
    length = jnp.sqrt(lax.optimization_barrier(jnp.sum(gradient * gradient, axis=0)))
    field = -gradient / jnp.maximum(length, 1.0)
    projected = lax.optimization_barrier(jnp.sum(gradients * field[None, :, :], axis=1))
    live_mask = jnp.arange(slots) < live_count
    weight = jnp.where(live_mask, area_dev, 0.0)
    terms = projected * weight[None, :]
    empty = jnp.zeros((lookup_table.shape[0],), jnp.float32)
    return empty.at[corner_ids.reshape(-1)].add(terms.reshape(-1))

def reference(heat, basis, area, corners, send_sub, send_pat, live_faces):
    patch_count = N_PATCH
    sub_count = N_SUB
    devices = patch_count * sub_count
    owned_heat = heat.reshape(patch_count, sub_count, V_DEV)
    group_lists = send_sub.reshape(patch_count, sub_count, S_SUB)
    group_values = jnp.take_along_axis(owned_heat, group_lists, axis=2).reshape(patch_count, 1, sub_count * S_SUB)
    group_values = jnp.broadcast_to(group_values, (patch_count, sub_count, sub_count * S_SUB))
    patch_lists = send_pat.reshape(2 * RADIUS, patch_count, sub_count, S_PAT)
    blocks = []
    for block_index, offset in enumerate(offset_list()):
        sent = jnp.take_along_axis(owned_heat, patch_lists[block_index], axis=2)
        blocks.append(jnp.roll(sent, offset, axis=0))
    patch_values = jnp.stack(blocks, axis=2).reshape(patch_count, sub_count, 2 * RADIUS * S_PAT)
    lookup_table = jnp.concatenate([owned_heat, group_values, patch_values], axis=2)
    table_len = lookup_table.shape[2]
    lookup_table = lookup_table.reshape(devices, table_len)
    corner_ids = corners.reshape(3, devices, F_DEV).transpose(1, 0, 2)
    basis_dev = basis.reshape(9, devices, F_DEV).transpose(1, 0, 2)
    area_dev = area.reshape(devices, F_DEV)
    table_sums = lax.map(lambda pack: face_terms(*pack), (lookup_table, corner_ids, basis_dev, area_dev, live_faces))
    table_sums = table_sums.reshape(patch_count, sub_count, table_len)
    result = table_sums[:, :, :V_DEV]
    start = V_DEV
    group_sums = table_sums[:, :, start:start + sub_count * S_SUB].reshape(patch_count, sub_count, sub_count, S_SUB)
    group_sums = lax.optimization_barrier(jnp.sum(group_sums, axis=1))
    patch_ids = jnp.arange(patch_count).astype(jnp.int32)[:, None, None]
    sub_ids = jnp.arange(sub_count).astype(jnp.int32)[None, :, None]
    result = result.at[patch_ids, sub_ids, group_lists].add(group_sums)
    start = V_DEV + sub_count * S_SUB
    patch_sums = table_sums[:, :, start:].reshape(patch_count, sub_count, 2 * RADIUS, S_PAT)
    for block_index, offset in enumerate(offset_list()):
        returned = jnp.roll(patch_sums[:, :, block_index], -offset, axis=0)
        result = result.at[patch_ids, sub_ids, patch_lists[block_index]].add(returned)
    return result.reshape(-1)
```

```python
import functools

import jax
import jax.numpy as jnp
from jax import lax
from jax.experimental import pallas as pl
from jax.experimental.pallas import tpu as pltpu
from jax.sharding import PartitionSpec as P

RADIUS = 2
LANES = 128
F32 = jnp.float32
BF16 = jnp.bfloat16


def offset_list():
    return [k + 1 for k in range(RADIUS)] + [-(k + 1) for k in range(RADIUS)]


def lane_pick(rows, lanes):
    return jnp.take_along_axis(rows, lanes, axis=1, mode="promise_in_bounds")


def split_two(x):
    high = x.astype(BF16).astype(F32)
    return high, x - high


def wide(row, count):
    return jnp.broadcast_to(row, (count, row.shape[1]))


def rows_dot(a, b):
    return lax.dot_general(a, b, (((1,), (1,)), ((), ())), preferred_element_type=F32)


def kernel(
    patch_count,
    sub_count,
    share,
    heat_ref,
    sends_ref,
    live_ref,
    basis_hbm,
    area_hbm,
    corners_hbm,
    out_ref,
    basis_in,
    area_in,
    corners_in,
    in_sem,
    padded,
    main,
    other,
    flat,
    grads,
    near_val,
    spot,
    parts,
    far,
    near_sum,
    send_group,
    send_patch,
    recv_group,
    recv_patch,
    back_group,
    back_patch,
    home_group,
    home_patch,
    sems_group,
    sems_patch,
    home_sems_group,
    home_sems_patch,
):
    p = lax.axis_index("patch")
    s = lax.axis_index("sub")
    offsets = offset_list()
    blocks = len(offsets)
    own_rows = heat_ref.shape[0]
    tiles = area_in.shape[0]
    groups = tiles // 8
    far_rows = far.shape[0]
    per_row = LANES // share
    group_rows = sub_count // per_row

    copies = [
        pltpu.make_async_copy(corners_hbm, corners_in, in_sem.at[0]),
        pltpu.make_async_copy(basis_hbm, basis_in, in_sem.at[1]),
        pltpu.make_async_copy(area_hbm, area_in, in_sem.at[2]),
    ]
    for copy in copies:
        copy.start()

    subs = [lax.rem(s + d, sub_count) for d in range(1, sub_count)]
    behind = [lax.rem(s + sub_count - d, sub_count) for d in range(1, sub_count)]
    ahead_patch = [lax.rem(p + o + patch_count, patch_count) for o in offsets]
    back_to = [lax.rem(p - o + patch_count, patch_count) for o in offsets]
    barrier = pltpu.get_barrier_semaphore()
    for target in subs:
        pl.semaphore_signal(barrier, inc=1, device_id={"patch": p, "sub": target})
    for target in ahead_patch:
        pl.semaphore_signal(barrier, inc=1, device_id={"patch": target, "sub": s})

    heat = heat_ref[...]
    piece_a, rest = split_two(heat)
    piece_b, piece_c = split_two(rest)
    pieces = jnp.concatenate([piece_a, piece_b, piece_c], axis=0).astype(BF16)
    lists = sends_ref[...]
    rows_of = lax.shift_right_logical(lists, 7).astype(F32)
    lanes_of = (lists & (LANES - 1)).astype(F32)
    row_iota = lax.broadcasted_iota(jnp.int32, (own_rows, LANES), 0).astype(F32)
    lane_iota = lax.broadcasted_iota(jnp.int32, (LANES, LANES), 0).astype(F32)
    for b in range(1 + blocks):
        hit = jnp.where(wide(rows_of[b : b + 1], own_rows) == row_iota, 1.0, 0.0)
        hit = jnp.concatenate([hit, hit, hit], axis=0).astype(BF16)
        table = lax.dot_general(
            pieces, hit, (((0,), (0,)), ((), ())), preferred_element_type=F32
        )
        picked = jnp.where(wide(lanes_of[b : b + 1], LANES) == lane_iota, table, 0.0)
        row = jnp.sum(picked, axis=0, keepdims=True)
        if b == 0:
            send_group[0] = row
        else:
            send_patch[b - 1] = row

    pl.semaphore_wait(barrier, sub_count - 1 + blocks)

    def to_sub(src, dst, send, recv, target):
        return pltpu.make_async_remote_copy(
            src_ref=src,
            dst_ref=dst,
            send_sem=send,
            recv_sem=recv,
            device_id={"patch": p, "sub": target},
        )

    def to_patch(src, dst, send, recv, target):
        return pltpu.make_async_remote_copy(
            src_ref=src,
            dst_ref=dst,
            send_sem=send,
            recv_sem=recv,
            device_id={"patch": target, "sub": s},
        )

    sent = []
    for j in range(blocks):
        copy = to_patch(
            send_patch.at[j],
            recv_patch.at[j],
            sems_patch.at[0, j],
            sems_patch.at[1, j],
            ahead_patch[j],
        )
        copy.start()
        sent.append(copy)
    for d, target in enumerate(subs):
        copy = to_sub(
            send_group.at[0],
            recv_group.at[s],
            sems_group.at[0, d],
            sems_group.at[1, s],
            target,
        )
        copy.start()
        sent.append(copy)

    lane8 = lax.broadcasted_iota(jnp.int32, (own_rows, LANES), 1)
    padded[...] = jnp.zeros_like(padded)
    padded[8 : 8 + own_rows] = heat
    before = padded[7 : 7 + own_rows]
    after = padded[9 : 9 + own_rows]
    main[pl.ds(0, own_rows, stride=2), :] = heat
    main[pl.ds(1, own_rows, stride=2), :] = heat
    other[pl.ds(0, own_rows, stride=2), :] = before
    other[pl.ds(1, own_rows, stride=2), :] = jnp.where(lane8 < LANES // 2, after, before)

    for copy in copies:
        copy.wait()
    sub8 = lax.broadcasted_iota(jnp.int32, (8, LANES), 0)

    def prepare(g, carry):
        first = pl.multiple_of(8 * g, 8)
        for i in range(8):
            cols = pl.ds(pl.multiple_of((first + i) * LANES, LANES), LANES)
            flat[16 * i : 16 * i + 9, :] = basis_in[:, cols].astype(F32)
            spot[16 * i : 16 * i + 3, :] = corners_in[:, cols]
        for r in range(9):
            grads[r, pl.ds(first, 8), :] = flat[pl.ds(r, 8, stride=16), :]
        mains = main[pl.ds(first, 8), :]
        others = other[pl.ds(first, 8), :]
        home = lax.shift_right_logical(first + sub8, 1)
        for k in range(3):
            pos = spot[pl.ds(k, 8, stride=16), :]
            lanes = pos & (LANES - 1)
            rows = lax.shift_right_logical(pos, 7)
            near_val[k, pl.ds(first, 8), :] = jnp.where(
                rows == home, lane_pick(mains, lanes), lane_pick(others, lanes)
            )
            parts[k, pl.ds(first, 8), :] = pos
        return carry

    lax.fori_loop(0, groups, prepare, 0)

    for d, source in enumerate(behind):
        to_sub(
            send_group.at[0],
            recv_group.at[source],
            sems_group.at[0, d],
            sems_group.at[1, source],
            source,
        ).wait_recv()
    for j in range(blocks):
        to_patch(
            send_patch.at[j],
            recv_patch.at[j],
            sems_patch.at[0, j],
            sems_patch.at[1, j],
            ahead_patch[j],
        ).wait_recv()
    recv_group[s] = send_group[0]
    lane1 = lax.broadcasted_iota(jnp.int32, (1, LANES), 1)
    for r in range(group_rows):
        row = recv_group[r * per_row]
        for q in range(1, per_row):
            moved = pltpu.roll(recv_group[r * per_row + q], q * share, 1)
            row = jnp.where(lane1 < q * share, row, moved)
        far[r : r + 1, :] = row
    for j in range(blocks):
        far[group_rows + j : group_rows + j + 1, :] = recv_patch[j]

    window_rows = 2
    windows = far_rows // window_rows
    even = jnp.concatenate([far[pl.ds(0, windows, stride=2), :]] * (8 // windows), axis=0)
    odd = jnp.concatenate([far[pl.ds(1, windows, stride=2), :]] * (8 // windows), axis=0)
    live = live_ref[0]
    lane_ids = lax.broadcasted_iota(jnp.int32, (8, LANES), 1)
    id_iota = lax.broadcasted_iota(jnp.int32, (16, LANES), 0).astype(F32).astype(BF16)
    hot_iota = lane_iota.astype(BF16)
    one = jnp.ones((16, LANES), BF16)
    zero = jnp.zeros((16, LANES), BF16)
    near_sum[...] = jnp.zeros_like(near_sum)

    def work(g, far_acc):
        first = pl.multiple_of(8 * g, 8)
        tile = pl.ds(first, 8)
        values, lanes, ids = [], [], []
        for k in range(3):
            pos = parts[k, tile, :]
            lane = pos & (LANES - 1)
            row = lax.shift_right_logical(pos, 7)
            remote = jnp.where((row & 1) == 0, lane_pick(even, lane), lane_pick(odd, lane))
            values.append(jnp.where(row >= own_rows, remote, near_val[k, tile, :]))
            lanes.append(lane.astype(F32))
            ids.append(
                jnp.where(row >= own_rows, row - own_rows, row - 4 * g + 1 + far_rows).astype(F32)
            )
        grad = [[grads[3 * k + c, tile, :] for c in range(3)] for k in range(3)]
        total = [sum(grad[k][c] * values[k] for k in range(3)) for c in range(3)]
        squared = total[0] * total[0] + total[1] * total[1] + total[2] * total[2]
        scale = -1.0 / jnp.maximum(jnp.sqrt(squared), 1.0)
        slot = (first + sub8) * LANES + lane_ids
        scale = scale * jnp.where(slot < live, area_in[tile, :], 0.0)
        tops, lows = [], []
        for k in range(3):
            term = (
                grad[k][0] * total[0] + grad[k][1] * total[1] + grad[k][2] * total[2]
            ) * scale
            high, low = split_two(term)
            tops.append(high)
            lows.append(low)
        acc = jnp.zeros((32, LANES), F32)
        for pair in range(4):
            left, right = [], []
            for i in (2 * pair, 2 * pair + 1):
                for k in range(3):
                    id_wide = wide(ids[k][i : i + 1], 16).astype(BF16)
                    top = wide(tops[k][i : i + 1], 16).astype(BF16)
                    low = wide(lows[k][i : i + 1], 16).astype(BF16)
                    mask = id_wide == id_iota
                    left.append(
                        jnp.concatenate([jnp.where(mask, top, zero), jnp.where(mask, low, zero)], axis=0)
                    )
                    lane_wide = wide(lanes[k][i : i + 1], 16).astype(BF16)
                    right.append(
                        jnp.concatenate(
                            [
                                jnp.where(lane_wide == hot_iota[16 * n : 16 * n + 16], one, zero)
                                for n in range(LANES // 16)
                            ],
                            axis=0,
                        )
                    )
            acc = acc + rows_dot(jnp.concatenate(left, axis=1), jnp.concatenate(right, axis=1))
        acc = acc[:16] + acc[16:]
        at = pl.ds(pl.multiple_of(4 * g, 4), 8)
        near_sum[at, :] = near_sum[at, :] + acc[8:]
        return far_acc + acc[:8]

    sums = lax.fori_loop(0, groups, work, jnp.zeros((8, LANES), F32))

    for target in range(sub_count):
        row = sums[target // per_row : target // per_row + 1]
        if per_row > 1:
            shift = (target % per_row) * share
            if shift:
                row = pltpu.roll(row, LANES - shift, 1)
            row = jnp.where(lane1 < share, row, 0.0)
        back_group[target] = row
    for j in range(blocks):
        back_patch[j] = sums[group_rows + j : group_rows + j + 1]
    for j in range(blocks):
        copy = to_patch(
            back_patch.at[j],
            home_patch.at[j],
            home_sems_patch.at[0, j],
            home_sems_patch.at[1, j],
            back_to[j],
        )
        copy.start()
        sent.append(copy)
    for d, target in enumerate(subs):
        copy = to_sub(
            back_group.at[target],
            home_group.at[s],
            home_sems_group.at[0, d],
            home_sems_group.at[1, s],
            target,
        )
        copy.start()
        sent.append(copy)
    hot = []
    for b in range(1 + blocks):
        lane_wide = wide(lanes_of[b : b + 1], LANES)
        hot.append(jnp.where(lane_wide == lane_iota, 1.0, 0.0).astype(BF16))
    hot = jnp.concatenate(hot, axis=1)

    for d, source in enumerate(behind):
        to_sub(
            back_group.at[source],
            home_group.at[source],
            home_sems_group.at[0, d],
            home_sems_group.at[1, source],
            source,
        ).wait_recv()
    for j in range(blocks):
        to_patch(
            back_patch.at[j],
            home_patch.at[j],
            home_sems_patch.at[0, j],
            home_sems_patch.at[1, j],
            back_to[j],
        ).wait_recv()
    total = back_group[s]
    for source in behind:
        total = total + home_group[source]
    returned = [total] + [home_patch[j] for j in range(blocks)]
    left = []
    for b in range(1 + blocks):
        hit = wide(rows_of[b : b + 1], own_rows) == row_iota
        high, low = split_two(returned[b])
        left.append(
            jnp.concatenate(
                [
                    jnp.where(hit, wide(high, own_rows), 0.0),
                    jnp.where(hit, wide(low, own_rows), 0.0),
                ],
                axis=0,
            ).astype(BF16)
        )
    added = rows_dot(jnp.concatenate(left, axis=1), hot)
    out_ref[...] = near_sum[1 : 1 + own_rows, :] + added[:own_rows] + added[own_rows:]
    for copy in sent:
        copy.wait_send()


def solution(mesh):
    patch_count, sub_count = mesh.shape["patch"], mesh.shape["sub"]

    def per_device(heat, basis, area, corners, send_sub, send_pat, live_faces):
        owned, slots = heat.shape[0], area.shape[0]
        share = send_sub.shape[0]
        blocks, block_size = send_pat.shape
        own_rows, tiles = owned // LANES, slots // LANES
        far_rows = (sub_count * share + blocks * block_size) // LANES
        assert block_size == LANES and LANES % share == 0 and far_rows == 8
        lists = jnp.concatenate([jnp.pad(send_sub, (0, LANES - share))[None], send_pat], axis=0)
        vmem = pl.BlockSpec(memory_space=pltpu.VMEM)
        hbm = pl.BlockSpec(memory_space=pl.ANY)
        row = (1, LANES)
        out = pl.pallas_call(
            functools.partial(kernel, patch_count, sub_count, share),
            out_shape=jax.ShapeDtypeStruct((own_rows, LANES), F32),
            in_specs=[vmem, vmem, pl.BlockSpec(memory_space=pltpu.SMEM), hbm, hbm, hbm],
            out_specs=vmem,
            scratch_shapes=[
                pltpu.VMEM(basis.shape, basis.dtype),
                pltpu.VMEM((tiles, LANES), F32),
                pltpu.VMEM(corners.shape, corners.dtype),
                pltpu.SemaphoreType.DMA((3,)),
                pltpu.VMEM((own_rows + 16, LANES), F32),
                pltpu.VMEM((tiles, LANES), F32),
                pltpu.VMEM((tiles, LANES), F32),
                pltpu.VMEM((LANES, LANES), F32),
                pltpu.VMEM((9, tiles, LANES), F32),
                pltpu.VMEM((3, tiles, LANES), F32),
                pltpu.VMEM((LANES, LANES), jnp.int32),
                pltpu.VMEM((3, tiles, LANES), jnp.int32),
                pltpu.VMEM((far_rows, LANES), F32),
                pltpu.VMEM((own_rows + 16, LANES), F32),
                pltpu.VMEM((1,) + row, F32),
                pltpu.VMEM((blocks,) + row, F32),
                pltpu.VMEM((sub_count,) + row, F32),
                pltpu.VMEM((blocks,) + row, F32),
                pltpu.VMEM((sub_count,) + row, F32),
                pltpu.VMEM((blocks,) + row, F32),
                pltpu.VMEM((sub_count,) + row, F32),
                pltpu.VMEM((blocks,) + row, F32),
                pltpu.SemaphoreType.DMA((2, sub_count)),
                pltpu.SemaphoreType.DMA((2, blocks)),
                pltpu.SemaphoreType.DMA((2, sub_count)),
                pltpu.SemaphoreType.DMA((2, blocks)),
            ],
            compiler_params=pltpu.CompilerParams(collective_id=0, has_side_effects=True),
            name="divergence",
        )(
            heat.reshape(own_rows, LANES),
            lists,
            live_faces,
            basis,
            area.reshape(tiles, LANES),
            corners,
        )
        return out.reshape(owned)

    placed = (
        P(("patch", "sub")),
        P(None, ("patch", "sub")),
        P(("patch", "sub")),
        P(None, ("patch", "sub")),
        P(("patch", "sub")),
        P(None, ("patch", "sub")),
        P(("patch", "sub")),
    )
    return jax.shard_map(
        per_device, mesh=mesh, in_specs=placed, out_specs=P(("patch", "sub")), check_vma=False
    )
```

```python
import functools

import jax
import jax.numpy as jnp
from jax import lax
from jax.experimental import pallas as pl
from jax.experimental.pallas import tpu as pltpu
from jax.sharding import PartitionSpec as P

RADIUS = 2
LANES = 128
HALF = 64
F32 = jnp.float32
BF16 = jnp.bfloat16


def offset_list():
    return [k + 1 for k in range(RADIUS)] + [-(k + 1) for k in range(RADIUS)]


def lane_pick(rows, lanes):
    return jnp.take_along_axis(rows, lanes, axis=1, mode="promise_in_bounds")


def split_two(x):
    high = x.astype(BF16).astype(F32)
    return high, x - high


def wide(row, count):
    return jnp.broadcast_to(row, (count, row.shape[1]))


def rows_dot(a, b):
    return lax.dot_general(a, b, (((1,), (1,)), ((), ())), preferred_element_type=F32)


def kernel(
    patch_count,
    sub_count,
    share,
    heat_hbm,
    sub_list_hbm,
    patch_list_hbm,
    live_hbm,
    basis_hbm,
    area_hbm,
    corners_hbm,
    out_ref,
    heat_ref,
    sub_list_ref,
    patch_list_ref,
    live_ref,
    basis_in,
    area_in,
    corners_in,
    in_sem,
    padded,
    main,
    other,
    flat,
    grads,
    near_val,
    spot,
    parts,
    terms,
    hot_mem,
    row_mem,
    far,
    far_sum,
    near_sum,
    send_group,
    send_patch,
    recv_group,
    recv_patch,
    back_group,
    back_patch,
    home_group,
    home_patch,
    sems_group,
    sems_patch,
    home_sems_group,
    home_sems_patch,
):
    p = lax.axis_index("patch")
    s = lax.axis_index("sub")
    offsets = offset_list()
    blocks = len(offsets)
    own_rows = heat_ref.shape[0]
    tiles = area_in.shape[0]
    groups = tiles // 8
    far_rows = far.shape[0]
    per_row = LANES // share
    group_rows = sub_count // per_row

    subs = [lax.rem(s + d, sub_count) for d in range(1, sub_count)]
    behind = [lax.rem(s + sub_count - d, sub_count) for d in range(1, sub_count)]
    ahead_patch = [lax.rem(p + o + patch_count, patch_count) for o in offsets]
    back_to = [lax.rem(p - o + patch_count, patch_count) for o in offsets]
    barrier = pltpu.get_barrier_semaphore()
    for target in subs:
        pl.semaphore_signal(barrier, inc=1, device_id={"patch": p, "sub": target})
    for target in ahead_patch:
        pl.semaphore_signal(barrier, inc=1, device_id={"patch": target, "sub": s})

    early = [
        pltpu.make_async_copy(heat_hbm, heat_ref, in_sem.at[0]),
        pltpu.make_async_copy(sub_list_hbm, sub_list_ref, in_sem.at[1]),
        pltpu.make_async_copy(patch_list_hbm, patch_list_ref, in_sem.at[2]),
    ]
    copies = [
        pltpu.make_async_copy(corners_hbm, corners_in, in_sem.at[3]),
        pltpu.make_async_copy(basis_hbm, basis_in, in_sem.at[4]),
        pltpu.make_async_copy(area_hbm, area_in, in_sem.at[5]),
        pltpu.make_async_copy(live_hbm, live_ref, in_sem.at[6]),
    ]
    for copy in early + copies:
        copy.start()

    for copy in early:
        copy.wait()
    heat = heat_ref[...]
    piece_a, rest = split_two(heat)
    piece_b, piece_c = split_two(rest)
    pieces = jnp.concatenate([piece_a, piece_b, piece_c], axis=0).astype(BF16)
    sub_list = sub_list_ref[...]
    if share < LANES:
        sub_list = jnp.concatenate([sub_list, jnp.zeros((1, LANES - share), jnp.int32)], axis=1)
    lists = jnp.concatenate([sub_list, patch_list_ref[...]], axis=0)
    rows_of = lax.shift_right_logical(lists, 7).astype(F32)
    lanes_of = (lists & (LANES - 1)).astype(F32)
    row_iota = lax.broadcasted_iota(jnp.int32, (own_rows, LANES), 0).astype(F32)
    lane_iota = lax.broadcasted_iota(jnp.int32, (LANES, LANES), 0).astype(F32)
    for b in range(1 + blocks):
        hit = jnp.where(wide(rows_of[b : b + 1], own_rows) == row_iota, 1.0, 0.0)
        hit = jnp.concatenate([hit, hit, hit], axis=0).astype(BF16)
        table = lax.dot_general(
            pieces, hit, (((0,), (0,)), ((), ())), preferred_element_type=F32
        )
        picked = jnp.where(wide(lanes_of[b : b + 1], LANES) == lane_iota, table, 0.0)
        row = jnp.sum(picked, axis=0, keepdims=True)
        if b == 0:
            send_group[0] = row
        else:
            send_patch[b - 1] = row

    pl.semaphore_wait(barrier, sub_count - 1 + blocks)

    def to_sub(src, dst, send, recv, target):
        return pltpu.make_async_remote_copy(
            src_ref=src,
            dst_ref=dst,
            send_sem=send,
            recv_sem=recv,
            device_id={"patch": p, "sub": target},
        )

    def to_patch(src, dst, send, recv, target):
        return pltpu.make_async_remote_copy(
            src_ref=src,
            dst_ref=dst,
            send_sem=send,
            recv_sem=recv,
            device_id={"patch": target, "sub": s},
        )

    sent = []
    for j in range(blocks):
        copy = to_patch(
            send_patch.at[j],
            recv_patch.at[j],
            sems_patch.at[0, j],
            sems_patch.at[1, j],
            ahead_patch[j],
        )
        copy.start()
        sent.append(copy)
    for d, target in enumerate(subs):
        copy = to_sub(
            send_group.at[0],
            recv_group.at[s],
            sems_group.at[0, d],
            sems_group.at[1, s],
            target,
        )
        copy.start()
        sent.append(copy)

    lane8 = lax.broadcasted_iota(jnp.int32, (own_rows, LANES), 1)
    padded[...] = jnp.zeros_like(padded)
    padded[8 : 8 + own_rows] = heat
    before = padded[7 : 7 + own_rows]
    after = padded[9 : 9 + own_rows]
    main[pl.ds(0, own_rows, stride=2), :] = heat
    main[pl.ds(1, own_rows, stride=2), :] = heat
    other[pl.ds(0, own_rows, stride=2), :] = before
    other[pl.ds(1, own_rows, stride=2), :] = jnp.where(lane8 < LANES // 2, after, before)

    for copy in copies:
        copy.wait()
    one = jnp.ones((16, LANES), BF16)
    zero = jnp.zeros((16, LANES), BF16)
    sub8 = lax.broadcasted_iota(jnp.int32, (8, LANES), 0)

    def prepare(g, carry):
        first = pl.multiple_of(8 * g, 8)
        for i in range(8):
            cols = pl.ds(pl.multiple_of((first + i) * LANES, LANES), LANES)
            flat[16 * i : 16 * i + 9, :] = basis_in[:, cols].astype(F32)
            spot[16 * i : 16 * i + 3, :] = corners_in[:, cols]
        for r in range(9):
            grads[r, pl.ds(first, 8), :] = flat[pl.ds(r, 8, stride=16), :]
        mains = main[pl.ds(first, 8), :]
        others = other[pl.ds(first, 8), :]
        home = lax.shift_right_logical(first + sub8, 1)
        for k in range(3):
            pos = spot[pl.ds(k, 8, stride=16), :]
            lanes = pos & (LANES - 1)
            rows = lax.shift_right_logical(pos, 7)
            near_val[k, pl.ds(first, 8), :] = jnp.where(
                rows == home, lane_pick(mains, lanes), lane_pick(others, lanes)
            )
            parts[k, pl.ds(first, 8), :] = pos
        return carry

    lax.fori_loop(0, groups, prepare, 0)

    id_iota = lax.broadcasted_iota(jnp.int32, (32, LANES), 0).astype(F32).astype(BF16)
    hot_iota = lane_iota[:HALF].astype(BF16)

    def encode(g, carry):
        tile = pl.ds(pl.multiple_of(8 * g, 8), 8)
        for k in range(3):
            pos = parts[k, tile, :]
            lanes = (pos & (HALF - 1)).astype(F32)
            rows = lax.shift_right_logical(pos, 6)
            ids = jnp.where(
                rows >= 2 * own_rows, rows - 2 * own_rows, rows - 8 * g + 2 + 2 * far_rows
            ).astype(F32)
            for i in range(8):
                cols = slice((3 * i + k) * LANES, (3 * i + k + 1) * LANES)
                lane_wide = wide(lanes[i : i + 1], 16).astype(BF16)
                for n in range(HALF // 16):
                    part = slice(16 * n, 16 * n + 16)
                    hot_mem[g, part, cols] = jnp.where(lane_wide == hot_iota[part], one, zero)
                id_wide = wide(ids[i : i + 1], 16).astype(BF16)
                for n in range(2):
                    part = slice(16 * n, 16 * n + 16)
                    row_mem[g, part, cols] = jnp.where(id_wide == id_iota[part], one, zero)
        return carry

    lax.fori_loop(0, groups, encode, 0)

    for d, source in enumerate(behind):
        to_sub(
            send_group.at[0],
            recv_group.at[source],
            sems_group.at[0, d],
            sems_group.at[1, source],
            source,
        ).wait_recv()
    for j in range(blocks):
        to_patch(
            send_patch.at[j],
            recv_patch.at[j],
            sems_patch.at[0, j],
            sems_patch.at[1, j],
            ahead_patch[j],
        ).wait_recv()
    recv_group[s] = send_group[0]
    lane1 = lax.broadcasted_iota(jnp.int32, (1, LANES), 1)
    for r in range(group_rows):
        row = recv_group[r * per_row]
        for q in range(1, per_row):
            moved = pltpu.roll(recv_group[r * per_row + q], q * share, 1)
            row = jnp.where(lane1 < q * share, row, moved)
        far[r : r + 1, :] = row
    for j in range(blocks):
        far[group_rows + j : group_rows + j + 1, :] = recv_patch[j]

    window_rows = 2
    windows = far_rows // window_rows
    even = jnp.concatenate([far[pl.ds(0, windows, stride=2), :]] * (8 // windows), axis=0)
    odd = jnp.concatenate([far[pl.ds(1, windows, stride=2), :]] * (8 // windows), axis=0)
    live = live_ref[0]
    lane_ids = lax.broadcasted_iota(jnp.int32, (8, LANES), 1)
    near_sum[...] = jnp.zeros_like(near_sum)

    def evaluate(g, carry):
        first = pl.multiple_of(8 * g, 8)
        tile = pl.ds(first, 8)
        values = []
        for k in range(3):
            pos = parts[k, tile, :]
            lane = pos & (LANES - 1)
            row = lax.shift_right_logical(pos, 7)
            remote = jnp.where((row & 1) == 0, lane_pick(even, lane), lane_pick(odd, lane))
            values.append(jnp.where(row >= own_rows, remote, near_val[k, tile, :]))
        grad = [[grads[3 * k + c, tile, :] for c in range(3)] for k in range(3)]
        total = [sum(grad[k][c] * values[k] for k in range(3)) for c in range(3)]
        squared = total[0] * total[0] + total[1] * total[1] + total[2] * total[2]
        scale = -1.0 / jnp.maximum(jnp.sqrt(squared), 1.0)
        slot = (first + sub8) * LANES + lane_ids
        scale = scale * jnp.where(slot < live, area_in[tile, :], 0.0)
        for k in range(3):
            term = (
                grad[k][0] * total[0] + grad[k][1] * total[1] + grad[k][2] * total[2]
            ) * scale
            high, low = split_two(term)
            terms[k, tile, :] = high
            terms[3 + k, tile, :] = low
        return carry

    lax.fori_loop(0, groups, evaluate, 0, unroll=4)

    def scatter(g, far_acc):
        first = pl.multiple_of(8 * g, 8)
        tile = pl.ds(first, 8)
        rows = [terms[k, tile, :] for k in range(6)]
        left = []
        for i in range(8):
            for k in range(3):
                cols = slice((3 * i + k) * LANES, (3 * i + k + 1) * LANES)
                top = wide(rows[k][i : i + 1], 16).astype(BF16)
                low = wide(rows[3 + k][i : i + 1], 16).astype(BF16)
                up, down = row_mem[g, :16, cols], row_mem[g, 16:, cols]
                left.append(
                    jnp.concatenate([up * top, down * top, up * low, down * low], axis=0)
                )
        acc = rows_dot(jnp.concatenate(left, axis=1), hot_mem[g])
        acc = acc[:32] + acc[32:]
        at = pl.ds(first, 16)
        near_sum[at, :HALF] = near_sum[at, :HALF] + acc[16:]
        return far_acc + acc[:16]

    far_sum[:, :HALF] = lax.fori_loop(0, groups, scatter, jnp.zeros((16, HALF), F32), unroll=4)
    lane8s = lax.broadcasted_iota(jnp.int32, (far_rows, LANES), 1)
    sums = jnp.where(
        lane8s < HALF,
        far_sum[pl.ds(0, far_rows, stride=2), :],
        pltpu.roll(far_sum[pl.ds(1, far_rows, stride=2), :], HALF, 1),
    )

    for target in range(sub_count):
        row = sums[target // per_row : target // per_row + 1]
        if per_row > 1:
            shift = (target % per_row) * share
            if shift:
                row = pltpu.roll(row, LANES - shift, 1)
            row = jnp.where(lane1 < share, row, 0.0)
        back_group[target] = row
    for j in range(blocks):
        back_patch[j] = sums[group_rows + j : group_rows + j + 1]
    for j in range(blocks):
        copy = to_patch(
            back_patch.at[j],
            home_patch.at[j],
            home_sems_patch.at[0, j],
            home_sems_patch.at[1, j],
            back_to[j],
        )
        copy.start()
        sent.append(copy)
    for d, target in enumerate(subs):
        copy = to_sub(
            back_group.at[target],
            home_group.at[s],
            home_sems_group.at[0, d],
            home_sems_group.at[1, s],
            target,
        )
        copy.start()
        sent.append(copy)
    hot = []
    for b in range(1 + blocks):
        lane_wide = wide(lanes_of[b : b + 1], LANES)
        hot.append(jnp.where(lane_wide == lane_iota, 1.0, 0.0).astype(BF16))
    hot = jnp.concatenate(hot, axis=1)

    near = jnp.where(
        lane8 < HALF,
        near_sum[pl.ds(2, own_rows, stride=2), :],
        pltpu.roll(near_sum[pl.ds(3, own_rows, stride=2), :], HALF, 1),
    )
    for d, source in enumerate(behind):
        to_sub(
            back_group.at[source],
            home_group.at[source],
            home_sems_group.at[0, d],
            home_sems_group.at[1, source],
            source,
        ).wait_recv()
    for j in range(blocks):
        to_patch(
            back_patch.at[j],
            home_patch.at[j],
            home_sems_patch.at[0, j],
            home_sems_patch.at[1, j],
            back_to[j],
        ).wait_recv()
    total = back_group[s]
    for source in behind:
        total = total + home_group[source]
    returned = [total] + [home_patch[j] for j in range(blocks)]
    left = []
    for b in range(1 + blocks):
        hit = wide(rows_of[b : b + 1], own_rows) == row_iota
        high, low = split_two(returned[b])
        left.append(
            jnp.concatenate(
                [
                    jnp.where(hit, wide(high, own_rows), 0.0),
                    jnp.where(hit, wide(low, own_rows), 0.0),
                ],
                axis=0,
            ).astype(BF16)
        )
    added = rows_dot(jnp.concatenate(left, axis=1), hot)
    out_ref[...] = near + added[:own_rows] + added[own_rows:]
    for copy in sent:
        copy.wait_send()


def solution(mesh):
    patch_count, sub_count = mesh.shape["patch"], mesh.shape["sub"]

    def per_device(heat, basis, area, corners, send_sub, send_pat, live_faces):
        owned, slots = heat.shape[0], area.shape[0]
        share = send_sub.shape[0]
        blocks, block_size = send_pat.shape
        own_rows, tiles = owned // LANES, slots // LANES
        far_rows = (sub_count * share + blocks * block_size) // LANES
        assert block_size == LANES and LANES % share == 0 and far_rows == 8
        vmem = pl.BlockSpec(memory_space=pltpu.VMEM)
        hbm = pl.BlockSpec(memory_space=pl.ANY)
        row = (1, LANES)
        out = pl.pallas_call(
            functools.partial(kernel, patch_count, sub_count, share),
            out_shape=pltpu.VMEM((own_rows, LANES), F32),
            in_specs=[hbm] * 7,
            out_specs=vmem,
            scratch_shapes=[
                pltpu.VMEM((own_rows, LANES), F32),
                pltpu.VMEM((1, share), jnp.int32),
                pltpu.VMEM(send_pat.shape, jnp.int32),
                pltpu.SMEM((1,), jnp.int32),
                pltpu.VMEM(basis.shape, basis.dtype),
                pltpu.VMEM((tiles, LANES), F32),
                pltpu.VMEM(corners.shape, corners.dtype),
                pltpu.SemaphoreType.DMA((7,)),
                pltpu.VMEM((own_rows + 16, LANES), F32),
                pltpu.VMEM((tiles, LANES), F32),
                pltpu.VMEM((tiles, LANES), F32),
                pltpu.VMEM((LANES, LANES), F32),
                pltpu.VMEM((9, tiles, LANES), F32),
                pltpu.VMEM((3, tiles, LANES), F32),
                pltpu.VMEM((LANES, LANES), jnp.int32),
                pltpu.VMEM((3, tiles, LANES), jnp.int32),
                pltpu.VMEM((6, tiles, LANES), F32),
                pltpu.VMEM((tiles // 8, HALF, 24 * LANES), BF16),
                pltpu.VMEM((tiles // 8, 32, 24 * LANES), BF16),
                pltpu.VMEM((far_rows, LANES), F32),
                pltpu.VMEM((2 * far_rows, LANES), F32),
                pltpu.VMEM((2 * own_rows + 16, LANES), F32),
                pltpu.VMEM((1,) + row, F32),
                pltpu.VMEM((blocks,) + row, F32),
                pltpu.VMEM((sub_count,) + row, F32),
                pltpu.VMEM((blocks,) + row, F32),
                pltpu.VMEM((sub_count,) + row, F32),
                pltpu.VMEM((blocks,) + row, F32),
                pltpu.VMEM((sub_count,) + row, F32),
                pltpu.VMEM((blocks,) + row, F32),
                pltpu.SemaphoreType.DMA((2, sub_count)),
                pltpu.SemaphoreType.DMA((2, blocks)),
                pltpu.SemaphoreType.DMA((2, sub_count)),
                pltpu.SemaphoreType.DMA((2, blocks)),
            ],
            compiler_params=pltpu.CompilerParams(collective_id=0, has_side_effects=True),
            name="divergence",
        )(
            heat.reshape(own_rows, LANES),
            send_sub.reshape(1, share),
            send_pat,
            live_faces,
            basis,
            area.reshape(tiles, LANES),
            corners,
        )
        return out.reshape(owned)

    placed = (
        P(("patch", "sub")),
        P(None, ("patch", "sub")),
        P(("patch", "sub")),
        P(None, ("patch", "sub")),
        P(("patch", "sub")),
        P(None, ("patch", "sub")),
        P(("patch", "sub")),
    )
    return jax.shard_map(
        per_device, mesh=mesh, in_specs=placed, out_specs=P(("patch", "sub")), check_vma=False
    )
```
